32 devices in a mesh: wide: 16 (over z, y, x), narrow: 2 (over core).
Axes of the slice: x: 2, y: 2, z: 4, core: 2. Of those that a mesh axis runs over, the one named last changes fastest.
Arguments:
- tokens: bfloat16 [32, 200, 768], P(('wide', 'narrow')), may hold values from -6 to 6
- memory_raw: bfloat16 [32, 896, 768], P(('wide', 'narrow')), may hold values from -22 to 22
- lengths: int32 [32], P(('wide', 'narrow')), may hold values from 5 to 200, as said below
- cotangent: bfloat16 [32, 200, 768], P(('wide', 'narrow')), may hold values from -6 to 6
- self_proj: bfloat16 [4, 768, 768], P(None, ('wide', 'narrow')), may hold values from -0.21875 to 0.21875
- cross_proj: bfloat16 [4, 768, 768], P(None, ('wide', 'narrow')), may hold values from -0.21875 to 0.21875
- ffn_pair: bfloat16 [2, 768, 3072], P(None, ('wide', 'narrow')), may hold values from -0.21875 to 0.21875
- ffn_gain: bfloat16 [3072], P(('wide', 'narrow')), may hold values from 0.5 to 1.5
- norm_gains: bfloat16 [5, 768], P(None, ('wide', 'narrow')), may hold values from 0.5 to 1.5
- rel_table: bfloat16 [512, 12], P(('wide', 'narrow')), may hold values from -5 to 5
- head_gain: bfloat16 [2, 12], replicated, may hold values from 0.099609375 to 1.8984375
- bn_scale: bfloat16 [768], P(('wide', 'narrow')), may hold values from 0.099609375 to 1.8984375
- bn_bias: bfloat16 [768], P(('wide', 'narrow')), may hold values from -3 to 3
Outputs:
- output: bfloat16 [32, 200, 768], P(('wide', 'narrow'))
- d_tokens: float32 [32, 200, 768], P(('wide', 'narrow'))
- d_memory: float32 [32, 896, 768], P(('wide', 'narrow'))
- d_self_proj: float32 [4, 768, 768], P(None, ('wide', 'narrow'))
- d_cross_proj: float32 [4, 768, 768], P(None, ('wide', 'narrow'))
- d_ffn_pair: float32 [2, 768, 3072], P(None, ('wide', 'narrow'))
- d_ffn_gain: float32 [3072], P(('wide', 'narrow'))
- d_norm_gains: float32 [5, 768], P(None, ('wide', 'narrow'))
- d_rel_table: float32 [512, 12], P(('wide', 'narrow'))
- d_head_gain: float32 [2, 12], replicated
- d_bn_scale: float32 [768], P(('wide', 'narrow'))
- d_bn_bias: float32 [768], P(('wide', 'narrow'))
The draws below stay inside these ranges and needn't reach their ends.
Inputs may be any that keep to these rules, and one draw needn't show every extreme that they name: `lengths`: some item has exactly 200 decoder tokens in every draw.
All inputs are finite; a program needn't handle non-finite values.
Results may differ from the reference program's by a relative error of at most 0.02.
Values may be sent and summed in bfloat16 or wider, within the bound.
A program may use at most 256 MiB of HBM per device.

```python
import math
import jax
import jax.numpy as jnp
import numpy as np
from jax import lax

D = 768
H = 12
FF = 3072
SEQ = 200
MEM = 896
NB = 512
ITEMS = 32


def draw_lengths(key, part):
    first_key, second_key = jax.random.split(key)
    drawn = jax.random.randint(first_key, (ITEMS,), 5, SEQ + 1, dtype=jnp.int32)
    longest = jax.random.randint(second_key, (), 0, ITEMS, dtype=jnp.int32)
    return jnp.where(jnp.arange(ITEMS, dtype=jnp.int32) == longest, SEQ, drawn).astype(jnp.int32)


def draw_memory_raw(key, part):
    subkeys = jax.random.split(jax.random.fold_in(key, 11), 2)
    channel_mean = jax.random.uniform(subkeys[0], (D,), jnp.float32, -1.0, 1.0)
    item_scale = 1.0 + 2.0 * jnp.arange(ITEMS, dtype=jnp.float32) / ITEMS
    noise = jnp.clip(jax.random.normal(subkeys[1], (ITEMS, MEM, D), jnp.float32), -6.0, 6.0)
    return (channel_mean + item_scale[:, None, None] * noise).astype(jnp.bfloat16)


def block_scale(rng, extent, shards, low, top_value):
    level = 1.0
    for dim, parts in shards:
        heights = jax.random.uniform(jax.random.fold_in(jax.random.fold_in(rng, 6), dim), (parts,), jnp.float32, low / len(shards), top_value / len(shards))
        level = level * jnp.repeat(jnp.exp(heights), extent[dim] // parts).reshape((-1,) + (1,) * (len(extent) - 1 - dim))
    return level


def scatter_about(key, dims, spread, reach, shards=(), kind=jnp.bfloat16):
    values = jax.random.normal(key, dims, jnp.float32) * spread
    if len(shards) > 0:
        values = block_scale(key, dims, shards, -0.22, 0.18) * values
    return jnp.clip(values, min=-reach, max=reach).astype(kind)


def setup_inputs(seed: int = 0) -> dict:
    key_of = jax.random.split(jax.random.key(seed), 14)
    return {
        "tokens": scatter_about(key_of[0], (ITEMS, SEQ, D), 1.0, 6.0, ((0, 32),)),
        "memory_raw": draw_memory_raw(jax.random.fold_in(key_of[13], 71), 0),
        "lengths": draw_lengths(jax.random.fold_in(key_of[13], 71), 0),
        "cotangent": scatter_about(key_of[3], (ITEMS, SEQ, D), 1.0, 6.0, ((0, 32),)),
        "self_proj": scatter_about(key_of[4], (4, D, D), D ** -0.5, 0.21875, ((1, 32),)),
        "cross_proj": scatter_about(key_of[5], (4, D, D), D ** -0.5, 0.21875, ((1, 32),)),
        "ffn_pair": scatter_about(key_of[6], (2, D, FF), D ** -0.5, 0.21875, ((1, 32),)),
        "ffn_gain": jnp.clip(1.0 + 0.1 * jax.random.normal(key_of[7], (FF,), jnp.float32), 0.5, 1.5).astype(jnp.bfloat16),
        "norm_gains": jnp.clip(1.0 + 0.1 * jax.random.normal(key_of[8], (5, D), jnp.float32), 0.5, 1.5).astype(jnp.bfloat16),
        "rel_table": scatter_about(key_of[9], (NB, H), 1.0, 5.0, ((0, 32),)),
        "head_gain": jnp.clip(1.0 + 0.18 * jax.random.normal(key_of[10], (2, H), jnp.float32), 0.099609375, 1.8984375).astype(jnp.bfloat16),
        "bn_scale": jnp.clip(1.0 + 0.18 * jax.random.normal(key_of[11], (D,), jnp.float32), 0.099609375, 1.8984375).astype(jnp.bfloat16),
        "bn_bias": scatter_about(key_of[12], (D,), 0.5, 3.0, ((0, 32),)),
    }


EPSILON = 1e-05
NEGATIVE = -1000000000.0
HIGHEST = lax.Precision.HIGHEST

@jax.custom_vjp
def low(v):
    return lax.optimization_barrier(v.astype(jnp.bfloat16)).astype(jnp.float32)

@jax.custom_vjp
def low_back(v):
    return v

def low_keep(v):
    return (low(v), None)

def low_pass(kept, grad):
    return (grad,)

def back_keep(v):
    return (v, None)

def back_low(kept, grad):
    return (low(grad),)
low.defvjp(low_keep, low_pass)
low_back.defvjp(back_keep, back_low)

def bucket_select(length, buckets):
    select = np.zeros((buckets, length), np.float32)
    for distance in range(length):
        if distance <= 128:
            bucket = 255 - distance
        else:
            scaled = math.log(distance / 128.0) / math.log(1023.0 / 128.0) * 127.0
            bucket = 255 - (int(math.ceil(scaled)) + 128)
        select[bucket, distance] = 1.0
    return select

def toeplitz(by_distance):
    head_count, row_count = by_distance.shape
    padded = jnp.concatenate([by_distance[:, ::-1], jnp.zeros_like(by_distance)], axis=1)
    repeated = jnp.tile(padded, (1, row_count))[:, :row_count * (2 * row_count - 1)]
    shaped = repeated.reshape(head_count, row_count, 2 * row_count - 1)
    return shaped[:, :, row_count - 1:]

def layer_norm(values, gain_row):
    centred = values - lax.optimization_barrier(jnp.mean(values, axis=-1, keepdims=True))
    variance = lax.optimization_barrier(jnp.mean(centred * centred, axis=-1, keepdims=True))
    return centred * lax.rsqrt(variance + EPSILON) * gain_row

def linear(values, weight):
    return jnp.einsum('...i,ij->...j', values, weight, precision=HIGHEST)

def split_heads(values, head_count):
    return values.reshape(values.shape[:-1] + (head_count, values.shape[-1] // head_count))

def attend(queries, key_rows, values, score_bias, allowed, head_scale):
    inv_root = 1.0 / math.sqrt(queries.shape[-1])
    scores = jnp.einsum('gqhe,gkhe->ghqk', queries, key_rows, precision=HIGHEST) * inv_root
    if score_bias is not None:
        scores = scores + score_bias
    scores = low_back(scores)
    if allowed is not None:
        scores = jnp.where(allowed, scores, NEGATIVE)
    maximum = lax.optimization_barrier(jnp.max(scores, axis=-1, keepdims=True))
    exponent = jnp.exp(scores - maximum)
    softmax_out = exponent / lax.optimization_barrier(jnp.sum(exponent, axis=-1, keepdims=True))
    attended = low_back(jnp.einsum('ghqk,gkhe->gqhe', low(softmax_out), values, precision=HIGHEST))
    scaled = low(attended * head_scale[:, None])
    return scaled.reshape(scaled.shape[:2] + (scaled.shape[2] * scaled.shape[3],))

def group_forward(params, tokens, memory_raw, lengths, bn_mean, inv_std):
    self_proj, cross_proj, ffn_pair, ffn_gain, norm_gains, rel_table, head_gain, bn_scale, bn_bias = params
    length = tokens.shape[1]
    head_count = head_gain.shape[1]
    select = jnp.asarray(bucket_select(length, rel_table.shape[0]), dtype=rel_table.dtype)
    score_bias = toeplitz(jnp.einsum('th,td->hd', rel_table, select, precision=HIGHEST))[None]
    positions = jnp.arange(length)
    causal = positions[None, :] <= positions[:, None]
    live_keys = positions[None, :] < lengths[:, None]
    allowed = causal[None, None] & live_keys[:, None, None, :]
    normed_one = low(layer_norm(tokens, norm_gains[0]))
    self_heads = [split_heads(low(low_back(linear(normed_one, self_proj[member]))), head_count) for member in range(3)]
    self_mixed = attend(self_heads[0], self_heads[1], self_heads[2], score_bias, allowed, head_gain[0])
    self_branch = low_back(linear(self_mixed, self_proj[3]))
    residual_one = tokens + layer_norm(self_branch, norm_gains[1])
    memory = low((memory_raw - bn_mean) * inv_std * bn_scale + bn_bias)
    normed_two = low(layer_norm(residual_one, norm_gains[2]))
    cross_query = split_heads(low(low_back(linear(normed_two, cross_proj[0]))), head_count)
    cross_key = split_heads(low(low_back(linear(memory, cross_proj[1]))), head_count)
    cross_value = split_heads(low(low_back(linear(memory, cross_proj[2]))), head_count)
    cross_mixed = attend(cross_query, cross_key, cross_value, None, None, head_gain[1])
    cross_branch = low_back(linear(cross_mixed, cross_proj[3]))
    residual_two = residual_one + layer_norm(cross_branch, norm_gains[3])
    normed_three = low(layer_norm(residual_two, norm_gains[4]))
    hidden = low_back(linear(normed_three, ffn_pair[0]))
    rescaled = low(layer_norm(jax.nn.gelu(hidden, approximate=False), ffn_gain))
    ffn_branch = low_back(jnp.einsum('gqf,df->gqd', rescaled, ffn_pair[1], precision=HIGHEST))
    return residual_two + ffn_branch

def forward(params, tokens, memory_raw, lengths):
    item_count = tokens.shape[0]
    group_size = math.gcd(item_count, 16)
    row_total = item_count * memory_raw.shape[1]
    bn_mean = lax.optimization_barrier(jnp.sum(memory_raw, axis=(0, 1))) / row_total
    variance = lax.optimization_barrier(jnp.sum(memory_raw * memory_raw, axis=(0, 1))) / row_total - bn_mean * bn_mean
    inv_std = lax.rsqrt(variance + EPSILON)

    def regroup(values):
        return values.reshape((item_count // group_size, group_size) + values.shape[1:])

    def one_group(pieces):
        return group_forward(params, pieces[0], pieces[1], pieces[2], bn_mean, inv_std)
    outputs = lax.map(jax.checkpoint(one_group), (regroup(tokens), regroup(memory_raw), regroup(lengths)))
    return outputs.reshape(tokens.shape)

def reference(tokens, memory_raw, lengths, cotangent, self_proj, cross_proj, ffn_pair, ffn_gain, norm_gains, rel_table, head_gain, bn_scale, bn_bias):
    params = tuple((argument.astype(jnp.float32) for argument in (self_proj, cross_proj, ffn_pair, ffn_gain, norm_gains, rel_table, head_gain, bn_scale, bn_bias)))

    def wrapped(weights, token_values, memory_values):
        return forward(weights, token_values, memory_values, lengths)
    outputs, pullback = jax.vjp(wrapped, params, tokens.astype(jnp.float32), memory_raw.astype(jnp.float32))
    weight_grads, token_grads, memory_grads = pullback(cotangent.astype(jnp.float32))
    return (outputs.astype(jnp.bfloat16), token_grads, memory_grads, weight_grads[0], weight_grads[1], weight_grads[2], weight_grads[3], weight_grads[4], weight_grads[5], weight_grads[6], weight_grads[7], weight_grads[8])
```

```python
from functools import partial
import math

import jax
import jax.numpy as jnp
import numpy as np
from jax import lax
from jax.experimental import pallas as pl
from jax.experimental.pallas import tpu as pltpu
from jax.sharding import PartitionSpec as P

EPSILON = 1e-05
NEGATIVE = -1000000000.0
HIGHEST = lax.Precision.HIGHEST
MESH = pl.DeviceIdType.MESH
W = 2
OA, OB = 2, 4
RB, RA, RZ = 1, 2, 3


def bucket_select(length, buckets):
    select = np.zeros((buckets, length), np.float32)
    for distance in range(length):
        if distance <= 128:
            bucket = 255 - distance
        else:
            scaled = math.log(distance / 128.0) / math.log(1023.0 / 128.0) * 127.0
            bucket = 255 - (int(math.ceil(scaled)) + 128)
        select[bucket, distance] = 1.0
    return select


def toeplitz(by_distance):
    head_count, row_count = by_distance.shape
    padded = jnp.concatenate([by_distance[:, ::-1], jnp.zeros_like(by_distance)], axis=1)
    repeated = jnp.tile(padded, (1, row_count))[:, : row_count * (2 * row_count - 1)]
    shaped = repeated.reshape(head_count, row_count, 2 * row_count - 1)
    return shaped[:, :, row_count - 1 :]


def norm_forward(values, gain_row):
    centred = values - jnp.mean(values, axis=-1, keepdims=True)
    variance = jnp.mean(centred * centred, axis=-1, keepdims=True)
    return centred * lax.rsqrt(variance + EPSILON) * gain_row


def norm_backward(values, gain_row, upstream):
    unused, pullback = jax.vjp(norm_forward, values, gain_row)
    return pullback(upstream)


def product(left_side, right_side):
    return jnp.dot(left_side, right_side, preferred_element_type=jnp.float32)


def back_product(upstream, weight):
    return jnp.einsum("ble,de->bld", upstream, weight, preferred_element_type=jnp.float32)


def weight_grad(activation, upstream):
    return jnp.einsum("bld,ble->de", activation, upstream, preferred_element_type=jnp.float32)


def to_heads(values, head_count):
    return values.reshape(
        values.shape[0], values.shape[1], head_count, values.shape[2] // head_count
    )


def from_heads(values):
    return values.reshape(values.shape[0], values.shape[1], values.shape[2] * values.shape[3])


def attend_scores(queries, key_rows, score_bias, allowed, inv_root):
    scores = (
        jnp.einsum("bqhe,bkhe->bhqk", queries, key_rows, preferred_element_type=jnp.float32)
        * inv_root
    )
    if score_bias is None:
        return scores
    return jnp.where(allowed, scores + score_bias, NEGATIVE)


def attend_forward(queries, key_rows, values, score_bias, allowed, head_scale, inv_root):
    scores = attend_scores(queries, key_rows, score_bias, allowed, inv_root)
    maximum = jnp.max(scores, axis=-1, keepdims=True)
    totals = maximum + jnp.log(jnp.sum(jnp.exp(scores - maximum), axis=-1, keepdims=True))
    softmax_low = jnp.exp(scores - totals).astype(jnp.bfloat16)
    attended = jnp.einsum(
        "bhqk,bkhe->bqhe", softmax_low, values, preferred_element_type=jnp.float32
    )
    scaled = (attended * head_scale[:, None]).astype(jnp.bfloat16)
    return (attended, from_heads(scaled), totals)


def attend_backward(
    queries, key_rows, values, score_bias, allowed, head_scale, inv_root, totals, attended, upstream
):
    head_grad = jnp.sum(upstream * attended, axis=(0, 1, 3))
    grad_attended = (upstream * head_scale[:, None]).astype(jnp.bfloat16)
    softmax_out = jnp.exp(attend_scores(queries, key_rows, score_bias, allowed, inv_root) - totals)
    softmax_low = softmax_out.astype(jnp.bfloat16)
    grad_soft = jnp.einsum(
        "bqhe,bkhe->bhqk", grad_attended, values, preferred_element_type=jnp.float32
    )
    grad_values = jnp.einsum(
        "bhqk,bqhe->bkhe", softmax_low, grad_attended, preferred_element_type=jnp.float32
    )
    grad_scores = softmax_out * (
        grad_soft - jnp.sum(softmax_out * grad_soft, axis=-1, keepdims=True)
    )
    grad_scores = grad_scores.astype(jnp.bfloat16)
    grad_queries = (
        jnp.einsum("bhqk,bkhe->bqhe", grad_scores, key_rows, preferred_element_type=jnp.float32)
        * inv_root
    )
    grad_keys = (
        jnp.einsum("bhqk,bqhe->bkhe", grad_scores, queries, preferred_element_type=jnp.float32)
        * inv_root
    )
    return (
        head_grad,
        grad_scores,
        from_heads(grad_queries.astype(jnp.bfloat16)),
        from_heads(grad_keys.astype(jnp.bfloat16)),
        from_heads(grad_values.astype(jnp.bfloat16)),
    )


def plain_body(
    tokens,
    memory_raw,
    lengths,
    cotangent,
    self_proj,
    cross_proj,
    ffn_pair,
    ffn_gain,
    norm_gains,
    rel_table,
    head_gain,
    bn_scale,
    bn_bias,
):
    item_count, length, model_width = tokens.shape
    head_count = head_gain.shape[1]
    inv_root = 1.0 / math.sqrt(model_width // head_count)
    mem_rows = memory_raw.shape[1]
    head_scales = head_gain.astype(jnp.float32)
    self_full, gains_full, table_full = (
        lax.all_gather(self_proj, ("wide", "narrow"), axis=1, tiled=True),
        lax.all_gather(norm_gains, ("wide", "narrow"), axis=1, tiled=True),
        lax.all_gather(rel_table, ("wide", "narrow"), axis=0, tiled=True),
    )
    norm_scale = gains_full.astype(jnp.float32)
    select = jnp.asarray(bucket_select(length, table_full.shape[0]))
    by_distance = jnp.einsum("th,td->hd", table_full.astype(jnp.float32), select, precision=HIGHEST)
    score_bias = toeplitz(by_distance)[None]
    positions = jnp.arange(length)
    causal = positions[None, :] <= positions[:, None]
    live_keys = positions[None, :] < lengths[:, None]
    allowed = causal[None, None] & live_keys[:, None, None, :]
    token_values = tokens.astype(jnp.float32)
    normed_one = norm_forward(token_values, norm_scale[0]).astype(jnp.bfloat16)
    self_queries = to_heads(product(normed_one, self_full[0]).astype(jnp.bfloat16), head_count)
    self_keys = to_heads(product(normed_one, self_full[1]).astype(jnp.bfloat16), head_count)
    self_values = to_heads(product(normed_one, self_full[2]).astype(jnp.bfloat16), head_count)
    self_attended, self_flat, self_totals = attend_forward(
        self_queries, self_keys, self_values, score_bias, allowed, head_scales[0], inv_root
    )
    self_branch = product(self_flat, self_full[3])
    residual_one = token_values + norm_forward(self_branch, norm_scale[1])
    cross_full, scale_full, shift_full = (
        lax.all_gather(cross_proj, ("wide", "narrow"), axis=1, tiled=True),
        lax.all_gather(bn_scale, ("wide", "narrow"), axis=0, tiled=True),
        lax.all_gather(bn_bias, ("wide", "narrow"), axis=0, tiled=True),
    )
    memory_values = memory_raw.astype(jnp.float32)
    plain_sum, square_sum = lax.psum(
        (jnp.sum(memory_values, axis=(0, 1)), jnp.sum(memory_values * memory_values, axis=(0, 1))),
        ("wide", "narrow"),
    )
    row_total = item_count * mem_rows * lax.axis_size(("wide", "narrow"))
    bn_mean = plain_sum / row_total
    inv_std = lax.rsqrt(square_sum / row_total - bn_mean * bn_mean + EPSILON)
    centred_mem = (memory_values - bn_mean) * inv_std
    bn_gain = scale_full.astype(jnp.float32)
    memory_low = (centred_mem * bn_gain + shift_full.astype(jnp.float32)).astype(jnp.bfloat16)
    normed_two = norm_forward(residual_one, norm_scale[2]).astype(jnp.bfloat16)
    cross_queries = to_heads(product(normed_two, cross_full[0]).astype(jnp.bfloat16), head_count)
    cross_keys = to_heads(product(memory_low, cross_full[1]).astype(jnp.bfloat16), head_count)
    cross_values = to_heads(product(memory_low, cross_full[2]).astype(jnp.bfloat16), head_count)
    cross_attended, cross_flat, cross_totals = attend_forward(
        cross_queries, cross_keys, cross_values, None, None, head_scales[1], inv_root
    )
    cross_branch = product(cross_flat, cross_full[3])
    residual_two = residual_one + norm_forward(cross_branch, norm_scale[3])
    ffn_full, ffn_scale = (
        lax.all_gather(ffn_pair, ("wide", "narrow"), axis=1, tiled=True),
        lax.all_gather(ffn_gain, ("wide", "narrow"), axis=0, tiled=True),
    )
    normed_three = norm_forward(residual_two, norm_scale[4]).astype(jnp.bfloat16)
    hidden = product(normed_three, ffn_full[0])
    activated = jax.nn.gelu(hidden, approximate=False)
    unit_scale = ffn_scale.astype(jnp.float32)
    rescaled = norm_forward(activated, unit_scale).astype(jnp.bfloat16)
    ffn_branch = jnp.einsum(
        "blf,df->bld", rescaled, ffn_full[1], preferred_element_type=jnp.float32
    )
    output = (residual_two + ffn_branch).astype(jnp.bfloat16)
    ffn_back = lax.all_gather(ffn_pair, ("wide", "narrow"), axis=1, tiled=True)
    upstream = cotangent.astype(jnp.float32)
    grad_rescaled = jnp.einsum(
        "bld,df->blf", cotangent, ffn_back[1], preferred_element_type=jnp.float32
    )
    grad_activated, grad_unit_scale = norm_backward(activated, unit_scale, grad_rescaled)
    unused, gelu_pull = jax.vjp(partial(jax.nn.gelu, approximate=False), hidden)
    grad_hidden = gelu_pull(grad_activated)[0].astype(jnp.bfloat16)
    grad_normed_three = jnp.einsum(
        "blf,df->bld", grad_hidden, ffn_back[0], preferred_element_type=jnp.float32
    )
    grad_two_part, grad_scale_four = norm_backward(residual_two, norm_scale[4], grad_normed_three)
    grad_res_two = upstream + grad_two_part
    grad_in = weight_grad(normed_three, grad_hidden)
    grad_out = weight_grad(cotangent, rescaled)
    ffn_grad_shard = jnp.transpose(
        lax.psum_scatter(
            jnp.stack([grad_in, grad_out], axis=1),
            ("wide", "narrow"),
            scatter_dimension=0,
            tiled=True,
        ),
        (1, 0, 2),
    )
    cross_back = lax.all_gather(cross_proj, ("wide", "narrow"), axis=1, tiled=True)
    grad_cross_branch, grad_scale_three = norm_backward(cross_branch, norm_scale[3], grad_res_two)
    grad_cross_low = grad_cross_branch.astype(jnp.bfloat16)
    grad_cross_scaled = to_heads(back_product(grad_cross_low, cross_back[3]), head_count)
    cross_head, unused_scores, grad_cross_query, grad_cross_key, grad_cross_value = attend_backward(
        cross_queries,
        cross_keys,
        cross_values,
        None,
        None,
        head_scales[1],
        inv_root,
        cross_totals,
        cross_attended,
        grad_cross_scaled,
    )
    grad_memory = back_product(grad_cross_key, cross_back[1]) + back_product(
        grad_cross_value, cross_back[2]
    )
    grad_one_part, grad_scale_two = norm_backward(
        residual_one, norm_scale[2], back_product(grad_cross_query, cross_back[0])
    )
    grad_res_one = grad_res_two + grad_one_part
    cross_grad_shard = jnp.transpose(
        lax.psum_scatter(
            jnp.stack(
                [
                    weight_grad(normed_two, grad_cross_query),
                    weight_grad(memory_low, grad_cross_key),
                    weight_grad(memory_low, grad_cross_value),
                    weight_grad(cross_flat, grad_cross_low),
                ],
                axis=1,
            ),
            ("wide", "narrow"),
            scatter_dimension=0,
            tiled=True,
        ),
        (1, 0, 2),
    )
    self_back = lax.all_gather(self_proj, ("wide", "narrow"), axis=1, tiled=True)
    grad_self_branch, grad_scale_one = norm_backward(self_branch, norm_scale[1], grad_res_one)
    grad_self_low = grad_self_branch.astype(jnp.bfloat16)
    grad_self_scaled = to_heads(back_product(grad_self_low, self_back[3]), head_count)
    self_head, grad_bias_scores, grad_self_query, grad_self_key, grad_self_value = attend_backward(
        self_queries,
        self_keys,
        self_values,
        score_bias,
        allowed,
        head_scales[0],
        inv_root,
        self_totals,
        self_attended,
        grad_self_scaled,
    )
    grad_bias = jnp.sum(grad_bias_scores.astype(jnp.float32), axis=0)
    unused_value, toeplitz_pull = jax.vjp(toeplitz, by_distance)
    grad_distance = toeplitz_pull(grad_bias)[0]
    grad_table = jnp.einsum("td,hd->th", select, grad_distance, precision=HIGHEST)
    grad_normed_one = (
        back_product(grad_self_query, self_back[0])
        + back_product(grad_self_key, self_back[1])
        + back_product(grad_self_value, self_back[2])
    )
    grad_tokens_part, grad_scale_zero = norm_backward(token_values, norm_scale[0], grad_normed_one)
    grad_tokens = grad_res_one + grad_tokens_part
    gain_grads = jnp.stack(
        [grad_scale_zero, grad_scale_one, grad_scale_two, grad_scale_three, grad_scale_four]
    )
    self_grad_shard = jnp.transpose(
        lax.psum_scatter(
            jnp.stack(
                [
                    weight_grad(normed_one, grad_self_query),
                    weight_grad(normed_one, grad_self_key),
                    weight_grad(normed_one, grad_self_value),
                    weight_grad(self_flat, grad_self_low),
                ],
                axis=1,
            ),
            ("wide", "narrow"),
            scatter_dimension=0,
            tiled=True,
        ),
        (1, 0, 2),
    )
    bias_part = jnp.sum(grad_memory, axis=(0, 1))
    scale_part = jnp.sum(grad_memory * centred_mem, axis=(0, 1))
    bn_totals, head_totals, gain_totals, table_totals, unit_totals = lax.psum(
        (
            jnp.stack([scale_part, bias_part]),
            jnp.stack([self_head, cross_head]),
            gain_grads,
            grad_table,
            grad_unit_scale,
        ),
        ("wide", "narrow"),
    )
    grad_memory_raw = (
        bn_gain
        * inv_std
        * (grad_memory - bn_totals[1] / row_total - centred_mem * (bn_totals[0] / row_total))
    )
    position = lax.axis_index(("wide", "narrow"))
    shard_width = bn_scale.shape[0]
    offset = position * shard_width
    bn_scale_shard = lax.dynamic_slice_in_dim(bn_totals[0], offset, shard_width)
    bn_bias_shard = lax.dynamic_slice_in_dim(bn_totals[1], offset, shard_width)
    gain_shard = lax.dynamic_slice_in_dim(gain_totals, offset, shard_width, 1)
    table_rows = rel_table.shape[0]
    table_shard = lax.dynamic_slice_in_dim(table_totals, position * table_rows, table_rows, 0)
    unit_width = ffn_gain.shape[0]
    ffn_gain_shard = lax.dynamic_slice_in_dim(unit_totals, position * unit_width, unit_width)
    return (
        output,
        grad_tokens,
        grad_memory_raw,
        self_grad_shard,
        cross_grad_shard,
        ffn_grad_shard,
        ffn_gain_shard,
        gain_shard,
        table_shard,
        head_totals,
        bn_scale_shard,
        bn_bias_shard,
    )


def place():
    w = lax.axis_index("wide"); c = lax.axis_index("narrow")
    z = w // 4; y = (w // 2) % 2; x = w % 2
    return w, c, z, y, x

def greet_all(w, c, nz):
    n = nz * 8
    sem = pltpu.get_barrier_semaphore()
    me = w * 2 + c
    def go(r, _):
        p = lax.rem(me + r, n)
        pl.semaphore_signal(sem, inc=1, device_id=(p // 2, p % 2), device_id_type=MESH)
        return 0
    lax.fori_loop(1, n, go, 0)
    pl.semaphore_wait(sem, n - 1)

def gather_kernel(nz, own_ref, small_ref, full_ref, smalls_ref,
                  zs, zr, as_, ar, bs, br, ds, dr, ls, ss, sr):
    U = own_ref.shape[0]
    w, c, z, y, x = place()
    n = nz * 8
    me = w * 2 + c
    ya, xa = (y + 1 - c) % 2, (x + c) % 2
    yb, xb = (y + c) % 2, (x + 1 - c) % 2
    wa = z * 4 + ya * 2 + xa
    wb = z * 4 + yb * 2 + xb
    greet_all(w, c, nz)
    loc = pltpu.make_async_copy(small_ref, smalls_ref.at[me], ls.at[U])
    loc.start()
    def small(r):
        p = lax.rem(me + r, n)
        return pltpu.make_async_remote_copy(small_ref, smalls_ref.at[me], ss.at[r], sr.at[n - r],
            device_id=(p // 2, p % 2), device_id_type=MESH)
    def sgo(r, _):
        small(r).start(); return 0
    lax.fori_loop(1, n, sgo, 0)

    def zcopy(u, r):
        t = lax.rem(z + r, nz)
        return pltpu.make_async_remote_copy(own_ref.at[u], full_ref.at[u, z, y, x, c],
            zs.at[u, r], zr.at[u, nz - r], device_id=(t * 4 + y * 2 + x, c), device_id_type=MESH)
    def lcopy(u):
        return pltpu.make_async_copy(own_ref.at[u], full_ref.at[u, z, y, x, c], ls.at[u])
    def acopy(u):
        blk = full_ref.at[u, :, y, x, c]
        return pltpu.make_async_remote_copy(blk, blk, as_.at[u], ar.at[u], device_id=(wa, c), device_id_type=MESH)
    def bcopy0(u):
        blk = full_ref.at[u, :, :, x, c]
        return pltpu.make_async_remote_copy(blk, blk, bs.at[u], br.at[u], device_id=(wb, c), device_id_type=MESH)
    def bcopy1(u):
        blk = full_ref.at[u, :, y, :, c]
        return pltpu.make_async_remote_copy(blk, blk, bs.at[u], br.at[u], device_id=(wb, c), device_id_type=MESH)
    def dcopy(u):
        blk = full_ref.at[u, :, :, :, c]
        return pltpu.make_async_remote_copy(blk, blk, ds.at[u], dr.at[u], device_id=(w, 1 - c), device_id_type=MESH)
    def start(u, _):
        lcopy(u).start()
        for r in range(1, nz):
            zcopy(u, r).start()
        return 0
    lax.fori_loop(0, min(W, U), start, 0)
    def tick(t, _):
        @pl.when(t + W < U)
        def _():
            start(t + W, 0)
        @pl.when(t < U)
        def _():
            lcopy(t).wait()
            for r in range(1, nz):
                zcopy(t, r).wait_recv()
            acopy(t).start()
        u1 = t - OA
        @pl.when(jnp.logical_and(u1 >= 0, u1 < U))
        def _():
            acopy(u1).wait_recv()
            @pl.when(c == 0)
            def _(): bcopy0(u1).start()
            @pl.when(c == 1)
            def _(): bcopy1(u1).start()
        u2 = t - OB
        @pl.when(u2 >= 0)
        def _():
            bcopy0(u2).wait_recv()
            dcopy(u2).start()
        return 0
    lax.fori_loop(0, U + OB, tick, 0)
    def drain(u, _):
        dcopy(u).wait_recv()
        dcopy(u).wait_send(); bcopy0(u).wait_send(); acopy(u).wait_send()
        for r in range(1, nz):
            zcopy(u, r).wait_send()
        return 0
    lax.fori_loop(0, U, drain, 0)
    loc.wait()
    def sw(r, _):
        small(r).wait(); return 0
    lax.fori_loop(1, n, sw, 0)

def gather(own, small, nz):
    U, rows, cols = own.shape
    n = nz * 8
    D = pltpu.SemaphoreType.DMA
    return pl.pallas_call(
        partial(gather_kernel, nz),
        out_shape=(jax.ShapeDtypeStruct((U, nz, 2, 2, 2, rows, cols), own.dtype),
                   jax.ShapeDtypeStruct((n,) + small.shape, small.dtype)),
        in_specs=[pl.BlockSpec(memory_space=pltpu.VMEM)] * 2,
        out_specs=(pl.BlockSpec(memory_space=pltpu.HBM), pl.BlockSpec(memory_space=pltpu.VMEM)),
        scratch_shapes=[D((U, nz)), D((U, nz)), D((U,)), D((U,)), D((U,)), D((U,)), D((U,)), D((U,)), D((U + 1,)), D((n,)), D((n + 1,))],
        compiler_params=pltpu.CompilerParams(collective_id=0, has_side_effects=True),
        name="gather",
    )(own, small)

def scatter_kernel(nz, g_ref, small_ref, out_ref, smalls_ref, rd, rb, ra, rz, ds, dr, bs, br, as_, ar, zs, zr, ls, ss, sr):
    U = g_ref.shape[0]
    w, c, z, y, x = place()
    ya, xa = (y + 1 - c) % 2, (x + c) % 2
    yb, xb = (y + c) % 2, (x + 1 - c) % 2
    wa = z * 4 + ya * 2 + xa
    wb = z * 4 + yb * 2 + xb
    n = nz * 8
    me = w * 2 + c
    greet_all(w, c, nz)
    loc = pltpu.make_async_copy(small_ref.at[me], smalls_ref.at[me], ls)
    loc.start()
    def small(r):
        p = lax.rem(me + r, n)
        return pltpu.make_async_remote_copy(small_ref.at[p], smalls_ref.at[me], ss.at[r], sr.at[n - r],
            device_id=(p // 2, p % 2), device_id_type=MESH)
    def sgo(r, _):
        small(r).start(); return 0
    lax.fori_loop(1, n, sgo, 0)
    f32 = jnp.float32
    def dcopy(u):
        return pltpu.make_async_remote_copy(g_ref.at[u, :, :, :, 1 - c], rd.at[u], ds.at[u], dr.at[u],
            device_id=(w, 1 - c), device_id_type=MESH)
    def bcopy0(u):
        return pltpu.make_async_remote_copy(rd.at[u, :, :, xb], rb.at[u], bs.at[u], br.at[u], device_id=(wb, c), device_id_type=MESH)
    def bcopy1(u):
        return pltpu.make_async_remote_copy(rd.at[u, :, yb], rb.at[u], bs.at[u], br.at[u], device_id=(wb, c), device_id_type=MESH)
    def acopy(u):
        other = jnp.where(c == 0, ya, xa)
        return pltpu.make_async_remote_copy(rb.at[u, :, other], ra.at[u], as_.at[u], ar.at[u], device_id=(wa, c), device_id_type=MESH)
    def zcopy(u, r):
        t = lax.rem(z + r, nz)
        return pltpu.make_async_remote_copy(ra.at[u, t], rz.at[u, nz - r], zs.at[u, r], zr.at[u, nz - r],
            device_id=(t * 4 + y * 2 + x, c), device_id_type=MESH)
    def start(u, _):
        dcopy(u).start(); return 0
    lax.fori_loop(0, min(W, U), start, 0)
    def tick(t, _):
        @pl.when(t + W < U)
        def _():
            start(t + W, 0)
        @pl.when(t < U)
        def _():
            dcopy(t).wait_recv()
            rd[t] = (rd[t].astype(f32) + g_ref[t, :, :, :, c].astype(f32)).astype(rd.dtype)
            @pl.when(c == 0)
            def _(): bcopy0(t).start()
            @pl.when(c == 1)
            def _(): bcopy1(t).start()
        u1 = t - RB
        @pl.when(jnp.logical_and(u1 >= 0, u1 < U))
        def _():
            bcopy0(u1).wait_recv()
            @pl.when(c == 0)
            def _(): rb[u1] = (rb[u1].astype(f32) + rd[u1, :, :, x].astype(f32)).astype(rb.dtype)
            @pl.when(c == 1)
            def _(): rb[u1] = (rb[u1].astype(f32) + rd[u1, :, y].astype(f32)).astype(rb.dtype)
            acopy(u1).start()
        u2 = t - RA
        @pl.when(jnp.logical_and(u2 >= 0, u2 < U))
        def _():
            acopy(u2).wait_recv()
            mine = jnp.where(c == 0, y, x)
            ra[u2] = (ra[u2].astype(f32) + rb[u2, :, mine].astype(f32)).astype(ra.dtype)
            for r in range(1, nz):
                zcopy(u2, r).start()
        u3 = t - RZ
        @pl.when(u3 >= 0)
        def _():
            total = ra[u3, z].astype(f32)
            for r in range(1, nz):
                zcopy(u3, r).wait_recv()
            for r in range(1, nz):
                total = total + rz[u3, r].astype(f32)
            out_ref[u3] = total
        return 0
    lax.fori_loop(0, U + RZ, tick, 0)
    def drain(u, _):
        dcopy(u).wait_send(); bcopy0(u).wait_send(); acopy(u).wait_send()
        for r in range(1, nz):
            zcopy(u, r).wait_send()
        return 0
    lax.fori_loop(0, U, drain, 0)

    loc.wait()
    def sw(r, _):
        small(r).wait(); return 0
    lax.fori_loop(1, n, sw, 0)

def scatter(g, smalls, nz):
    U, _, _, _, _, rows, cols = g.shape
    D = pltpu.SemaphoreType.DMA
    V = pltpu.VMEM
    n = nz * 8
    return pl.pallas_call(
        partial(scatter_kernel, nz),
        out_shape=(jax.ShapeDtypeStruct((U, rows, cols), jnp.float32), jax.ShapeDtypeStruct(smalls.shape, smalls.dtype)),
        in_specs=[pl.BlockSpec(memory_space=pltpu.VMEM)] * 2,
        out_specs=(pl.BlockSpec(memory_space=pltpu.VMEM),) * 2,
        scratch_shapes=[V((U, nz, 2, 2, rows, cols), g.dtype), V((U, nz, 2, rows, cols), g.dtype),
                        V((U, nz, rows, cols), g.dtype), V((U, nz, rows, cols), g.dtype),
                        D((U,)), D((U,)), D((U,)), D((U,)), D((U,)), D((U,)), D((U, nz)), D((U, nz)),
                        D(()), D((n,)), D((n + 1,))],
        compiler_params=pltpu.CompilerParams(collective_id=1, has_side_effects=True, vmem_limit_bytes=60 * 1024 * 1024),
        name="scatter",
    )(g, smalls)


def fast_body(
    tokens,
    memory_raw,
    lengths,
    cotangent,
    self_proj,
    cross_proj,
    ffn_pair,
    ffn_gain,
    norm_gains,
    rel_table,
    head_gain,
    bn_scale,
    bn_bias,
):
    item_count, length, model_width = tokens.shape
    head_count = head_gain.shape[1]
    inv_root = 1.0 / math.sqrt(model_width // head_count)
    mem_rows = memory_raw.shape[1]
    head_scales = head_gain.astype(jnp.float32)
    nz = lax.axis_size("wide") // 4
    n_dev = nz * 8
    rows = bn_scale.shape[0]
    hidden_width = ffn_pair.shape[2]
    cuts = hidden_width // model_width
    own = jnp.concatenate(
        [self_proj, cross_proj]
        + [ffn_pair[m, :, j * model_width : (j + 1) * model_width][None] for m in range(2) for j in range(cuts)]
    )
    memory_values = memory_raw.astype(jnp.float32)
    stats = jnp.stack([jnp.sum(memory_values, axis=(0, 1)), jnp.sum(memory_values * memory_values, axis=(0, 1))])
    vectors = jnp.concatenate([norm_gains.reshape(-1), rel_table.reshape(-1), ffn_gain, bn_scale, bn_bias]).astype(jnp.float32)
    pad = (-vectors.shape[0]) % 128
    vectors = jnp.pad(vectors, (0, pad))
    small = jnp.concatenate([vectors.reshape(-1, 128), stats.reshape(-1, 128)])
    full, smalls = gather(own, small, nz)
    full = full.reshape(own.shape[0], model_width, model_width)
    self_full = full[:4]
    cross_full = full[4:8]
    ffn_in = full[8 : 8 + cuts]
    ffn_out = full[8 + cuts :]
    vrows = (vectors.shape[0]) // 128
    flat = smalls[:, :vrows].reshape(n_dev, -1)
    at = 5 * rows
    gains_full = flat[:, :at].reshape(n_dev, 5, rows).transpose(1, 0, 2).reshape(5, model_width)
    tr = rel_table.shape[0]
    table_full = flat[:, at : at + tr * head_count].reshape(n_dev * tr, head_count)
    at += tr * head_count
    ffn_scale = flat[:, at : at + ffn_gain.shape[0]].reshape(-1)
    at += ffn_gain.shape[0]
    scale_full = flat[:, at : at + rows].reshape(-1)
    shift_full = flat[:, at + rows : at + 2 * rows].reshape(-1)
    stat_sums = jnp.sum(smalls[:, vrows:], axis=0).reshape(2, model_width)
    norm_scale = gains_full.astype(jnp.float32)
    select = jnp.asarray(bucket_select(length, table_full.shape[0]))
    by_distance = jnp.einsum("th,td->hd", table_full.astype(jnp.float32), select, precision=HIGHEST)
    score_bias = toeplitz(by_distance)[None]
    positions = jnp.arange(length)
    causal = positions[None, :] <= positions[:, None]
    live_keys = positions[None, :] < lengths[:, None]
    allowed = causal[None, None] & live_keys[:, None, None, :]
    token_values = tokens.astype(jnp.float32)
    normed_one = norm_forward(token_values, norm_scale[0]).astype(jnp.bfloat16)
    self_queries = to_heads(product(normed_one, self_full[0]).astype(jnp.bfloat16), head_count)
    self_keys = to_heads(product(normed_one, self_full[1]).astype(jnp.bfloat16), head_count)
    self_values = to_heads(product(normed_one, self_full[2]).astype(jnp.bfloat16), head_count)
    self_attended, self_flat, self_totals = attend_forward(
        self_queries, self_keys, self_values, score_bias, allowed, head_scales[0], inv_root
    )
    self_branch = product(self_flat, self_full[3])
    residual_one = token_values + norm_forward(self_branch, norm_scale[1])
    plain_sum, square_sum = stat_sums[0], stat_sums[1]
    row_total = item_count * mem_rows * lax.axis_size(("wide", "narrow"))
    bn_mean = plain_sum / row_total
    inv_std = lax.rsqrt(square_sum / row_total - bn_mean * bn_mean + EPSILON)
    centred_mem = (memory_values - bn_mean) * inv_std
    bn_gain = scale_full.astype(jnp.float32)
    memory_low = (centred_mem * bn_gain + shift_full.astype(jnp.float32)).astype(jnp.bfloat16)
    normed_two = norm_forward(residual_one, norm_scale[2]).astype(jnp.bfloat16)
    cross_queries = to_heads(product(normed_two, cross_full[0]).astype(jnp.bfloat16), head_count)
    cross_keys = to_heads(product(memory_low, cross_full[1]).astype(jnp.bfloat16), head_count)
    cross_values = to_heads(product(memory_low, cross_full[2]).astype(jnp.bfloat16), head_count)
    cross_attended, cross_flat, cross_totals = attend_forward(
        cross_queries, cross_keys, cross_values, None, None, head_scales[1], inv_root
    )
    cross_branch = product(cross_flat, cross_full[3])
    residual_two = residual_one + norm_forward(cross_branch, norm_scale[3])
    normed_three = norm_forward(residual_two, norm_scale[4]).astype(jnp.bfloat16)
    hidden = jnp.concatenate([product(normed_three, ffn_in[j]) for j in range(cuts)], axis=-1)
    activated = jax.nn.gelu(hidden, approximate=False)
    unit_scale = ffn_scale.astype(jnp.float32)
    rescaled = norm_forward(activated, unit_scale).astype(jnp.bfloat16)
    def piece(values, j):
        return values[:, :, j * model_width : (j + 1) * model_width]

    ffn_branch = sum(back_product(piece(rescaled, j), ffn_out[j]) for j in range(cuts))
    output = (residual_two + ffn_branch).astype(jnp.bfloat16)
    upstream = cotangent.astype(jnp.float32)
    grad_rescaled = jnp.concatenate([product(cotangent, ffn_out[j]) for j in range(cuts)], axis=-1)
    grad_activated, grad_unit_scale = norm_backward(activated, unit_scale, grad_rescaled)
    unused, gelu_pull = jax.vjp(partial(jax.nn.gelu, approximate=False), hidden)
    grad_hidden = gelu_pull(grad_activated)[0].astype(jnp.bfloat16)
    grad_normed_three = sum(back_product(piece(grad_hidden, j), ffn_in[j]) for j in range(cuts))
    grad_two_part, grad_scale_four = norm_backward(residual_two, norm_scale[4], grad_normed_three)
    grad_res_two = upstream + grad_two_part
    ffn_grads = [weight_grad(normed_three, piece(grad_hidden, j)) for j in range(cuts)] + [
        weight_grad(cotangent, piece(rescaled, j)) for j in range(cuts)
    ]
    cross_back = cross_full
    grad_cross_branch, grad_scale_three = norm_backward(cross_branch, norm_scale[3], grad_res_two)
    grad_cross_low = grad_cross_branch.astype(jnp.bfloat16)
    grad_cross_scaled = to_heads(back_product(grad_cross_low, cross_back[3]), head_count)
    cross_head, unused_scores, grad_cross_query, grad_cross_key, grad_cross_value = attend_backward(
        cross_queries,
        cross_keys,
        cross_values,
        None,
        None,
        head_scales[1],
        inv_root,
        cross_totals,
        cross_attended,
        grad_cross_scaled,
    )
    grad_memory = back_product(grad_cross_key, cross_back[1]) + back_product(
        grad_cross_value, cross_back[2]
    )
    grad_one_part, grad_scale_two = norm_backward(
        residual_one, norm_scale[2], back_product(grad_cross_query, cross_back[0])
    )
    grad_res_one = grad_res_two + grad_one_part
    cross_grads = [
        weight_grad(normed_two, grad_cross_query),
        weight_grad(memory_low, grad_cross_key),
        weight_grad(memory_low, grad_cross_value),
        weight_grad(cross_flat, grad_cross_low),
    ]
    self_back = self_full
    grad_self_branch, grad_scale_one = norm_backward(self_branch, norm_scale[1], grad_res_one)
    grad_self_low = grad_self_branch.astype(jnp.bfloat16)
    grad_self_scaled = to_heads(back_product(grad_self_low, self_back[3]), head_count)
    self_head, grad_bias_scores, grad_self_query, grad_self_key, grad_self_value = attend_backward(
        self_queries,
        self_keys,
        self_values,
        score_bias,
        allowed,
        head_scales[0],
        inv_root,
        self_totals,
        self_attended,
        grad_self_scaled,
    )
    grad_bias = jnp.sum(grad_bias_scores.astype(jnp.float32), axis=0)
    unused_value, toeplitz_pull = jax.vjp(toeplitz, by_distance)
    grad_distance = toeplitz_pull(grad_bias)[0]
    grad_table = jnp.einsum("td,hd->th", select, grad_distance, precision=HIGHEST)
    grad_normed_one = (
        back_product(grad_self_query, self_back[0])
        + back_product(grad_self_key, self_back[1])
        + back_product(grad_self_value, self_back[2])
    )
    grad_tokens_part, grad_scale_zero = norm_backward(token_values, norm_scale[0], grad_normed_one)
    grad_tokens = grad_res_one + grad_tokens_part
    gain_grads = jnp.stack(
        [grad_scale_zero, grad_scale_one, grad_scale_two, grad_scale_three, grad_scale_four]
    )
    self_grads = [
        weight_grad(normed_one, grad_self_query),
        weight_grad(normed_one, grad_self_key),
        weight_grad(normed_one, grad_self_value),
        weight_grad(self_flat, grad_self_low),
    ]
    bias_part = jnp.sum(grad_memory, axis=(0, 1))
    scale_part = jnp.sum(grad_memory * centred_mem, axis=(0, 1))
    owned = jnp.concatenate(
        [
            gain_grads.reshape(5, n_dev, rows).transpose(1, 0, 2).reshape(n_dev, -1),
            grad_table.reshape(n_dev, -1),
            grad_unit_scale.reshape(n_dev, -1),
        ],
        axis=1,
    )
    pad = (-owned.shape[1]) % 128
    owned = jnp.pad(owned, ((0, 0), (0, pad)))
    shared = jnp.concatenate([scale_part, bias_part, self_head, cross_head])
    shared = jnp.pad(shared, (0, (-shared.shape[0]) % 128))
    sent = jnp.concatenate([owned, jnp.broadcast_to(shared, (n_dev,) + shared.shape)], axis=1).reshape(n_dev, -1, 128)
    grads = jnp.stack([g.astype(jnp.bfloat16) for g in self_grads + cross_grads + ffn_grads])
    grads = grads.reshape(grads.shape[0], nz, 2, 2, 2, rows, model_width)
    shards, got = scatter(grads, sent, nz)
    got = jnp.sum(got, axis=0).reshape(-1)
    at = owned.shape[1]
    bn_totals = got[at : at + 2 * model_width].reshape(2, model_width)
    at += 2 * model_width
    head_totals = got[at : at + 2 * head_count].reshape(2, head_count)
    self_grad_shard = shards[:4]
    cross_grad_shard = shards[4:8]
    ffn_grad_shard = jnp.stack(
        [jnp.concatenate([shards[8 + m * cuts + j] for j in range(cuts)], axis=1) for m in range(2)]
    )
    grad_memory_raw = (
        bn_gain
        * inv_std
        * (grad_memory - bn_totals[1] / row_total - centred_mem * (bn_totals[0] / row_total))
    )
    position = lax.axis_index(("wide", "narrow"))
    shard_width = bn_scale.shape[0]
    offset = position * shard_width
    bn_scale_shard = lax.dynamic_slice_in_dim(bn_totals[0], offset, shard_width)
    bn_bias_shard = lax.dynamic_slice_in_dim(bn_totals[1], offset, shard_width)
    gain_shard = got[: 5 * rows].reshape(5, rows)
    at = 5 * rows
    table_shard = got[at : at + tr * head_count].reshape(tr, head_count)
    at += tr * head_count
    ffn_gain_shard = got[at : at + ffn_gain.shape[0]]
    return (
        output,
        grad_tokens,
        grad_memory_raw,
        self_grad_shard,
        cross_grad_shard,
        ffn_grad_shard,
        ffn_gain_shard,
        gain_shard,
        table_shard,
        head_totals,
        bn_scale_shard,
        bn_bias_shard,
    )


def solution(mesh):
    wide, narrow = mesh.shape["wide"], mesh.shape["narrow"]

    def body(*args):
        tokens, self_proj = args[0], args[4]
        fits = narrow == 2 and wide % 4 == 0 and self_proj.shape[1] % 8 == 0 and tokens.shape[0] == 1
        return (fast_body if fits else plain_body)(*args)

    return jax.shard_map(
        body,
        mesh=mesh,
        in_specs=(
            P(("wide", "narrow"), None, None),
            P(("wide", "narrow"), None, None),
            P(("wide", "narrow")),
            P(("wide", "narrow"), None, None),
            P(None, ("wide", "narrow"), None),
            P(None, ("wide", "narrow"), None),
            P(None, ("wide", "narrow"), None),
            P(("wide", "narrow")),
            P(None, ("wide", "narrow")),
            P(("wide", "narrow"), None),
            P(),
            P(("wide", "narrow")),
            P(("wide", "narrow")),
        ),
        out_specs=(
            P(("wide", "narrow"), None, None),
            P(("wide", "narrow"), None, None),
            P(("wide", "narrow"), None, None),
            P(None, ("wide", "narrow"), None),
            P(None, ("wide", "narrow"), None),
            P(None, ("wide", "narrow"), None),
            P(("wide", "narrow")),
            P(None, ("wide", "narrow")),
            P(("wide", "narrow"), None),
            P(),
            P(("wide", "narrow")),
            P(("wide", "narrow")),
        ),
        check_vma=False,
    )
```
